32 devices in a mesh: group: 2 (over y), seq: 4 (over x, core), dom: 4 (over z).
Axes of the slice: x: 2, y: 2, z: 4, core: 2. Of those that a mesh axis runs over, the one named last changes fastest.
Arguments:
- q_nope: bfloat16 [32, 128, 128], P(('group', 'dom'), 'seq'), parts along dimension 0, may hold values from -6 to 6
- q_rope: bfloat16 [32, 128, 64], P(('group', 'dom'), 'seq'), parts along dimension 0, may hold values from -8 to 8
- w_uk: bfloat16 [128, 128, 512], P('seq'), may hold values from -0.5 to 0.5
- w_uv: bfloat16 [128, 512, 128], P('seq'), may hold values from -1.5 to 1.5
- prefix: bfloat16 [32768, 576], P(('group', 'seq')), parts along dimension 0, may hold values from -8 to 8
- private_caches: bfloat16 [32, 256, 576], P(('group', 'dom'), 'seq'), parts along dimension 0, may hold values from -8 to 8
- new_latent: bfloat16 [32, 576], P(('group', 'dom')), parts along dimension 0, may hold values from -6 to 6
- ancestors: int32 [32], P(('group', 'dom')), parts along dimension 0, may hold values from 0 to 15
- lengths: int32 [32], P('group'), parts along dimension 0, may hold values from 1 to 255
Outputs:
- head_values: bfloat16 [32, 128, 128], P(('group', 'dom'), 'seq'), parts along dimension 0
- new_caches: bfloat16 [32, 256, 576], P(('group', 'dom'), 'seq'), parts along dimension 0
The draws below stay inside these ranges and needn't reach their ends.
There are 2 independent parts, one for each index of `group`. The reference program is written for one: setup_inputs(seed, part) draws one part's arguments, and reference() takes and returns one part's arrays. A program takes and returns all parts, laid end to end along the dimension named above; an argument that names none is the same for every part. Nothing has to cross between parts.
All inputs are finite; a program needn't handle non-finite values.
Results may differ from the reference program's by a relative error of at most 0.0085.
Values may be sent and summed in bfloat16 or wider, within the bound.
A program may use at most 64 MiB of HBM per device.

```python
import jax
import jax.numpy as jnp
from jax import lax

KV_RANK = 512
ROPE = 64
NOPE = 128
VH = 128
HEADS = 128
PRE_DEV = 4096
SUF_DEV = 64
PARTICLES = 16
PRE = 16384
SUF = 256
LATENT = 576
N_SEQ = 4


def draw_prefix(key, part):
    values = jnp.clip(1.5 * jax.random.normal(jax.random.fold_in(key, 11), (PRE, KV_RANK + ROPE), jnp.float32), -8.0, 8.0)
    return values.astype(jnp.bfloat16)


def draw_q_rope(key, part):
    values = jnp.clip(jax.random.normal(jax.random.fold_in(key, 17), (PARTICLES, HEADS, ROPE), jnp.float32), -8.0, 8.0)
    return values.astype(jnp.bfloat16)


def set_ends(result, stream_key, least, high):
    longest = result.shape.index(max(result.shape))
    spots = []
    for shift in (0, 1):
        where = [jax.random.randint(jax.random.fold_in(stream_key, axis), (), 0, length) for axis, length in enumerate(result.shape)]
        where[longest] = (where[longest] + shift) % result.shape[longest]
        spots.append(tuple(where))
    return result.at[spots[0]].set(least).at[spots[1]].set(high)


def steps_of(stream_key, dims, cuts, smallest, top_value):
    def one(axis_at, shards_of):
        heights = jax.random.uniform(jax.random.fold_in(jax.random.fold_in(stream_key, 6), axis_at), (shards_of,), jnp.float32, smallest / len(cuts), top_value / len(cuts))
        return jnp.repeat(jnp.exp(heights), dims[axis_at] // shards_of).reshape((-1,) + (1,) * (len(dims) - axis_at - 1))

    loudness = one(*cuts[0])
    for cut in cuts[1:]:
        loudness = loudness * one(*cut)
    return loudness


def noise(key, shape, deviation, reach, shards=(), kind=jnp.bfloat16):
    values = jax.random.normal(key, shape, jnp.float32) * deviation
    if len(shards) > 0:
        values = steps_of(key, shape, shards, -0.22, 0.18) * values
    return jnp.clip(values, min=-reach, max=reach).astype(kind)


def setup_inputs(seed: int = 0, part: int = 0) -> dict:
    key_list = jax.random.split(jax.random.key(seed), 10)
    part_splits = jax.random.split(jax.random.fold_in(key_list[9], part), 10)
    return {
        "q_nope": noise(part_splits[0], (PARTICLES, HEADS, NOPE), 1.0, 6.0, ((0, 4), (1, 4))),
        "q_rope": draw_q_rope(jax.random.fold_in(jax.random.fold_in(key_list[9], part), 71), part),
        "w_uk": noise(key_list[2], (HEADS, NOPE, KV_RANK), NOPE ** -0.5, 0.5, ((0, 4),)),
        "w_uv": noise(key_list[3], (HEADS, KV_RANK, VH), (KV_RANK // 32) ** -0.5, 1.5, ((0, 4),)),
        "prefix": draw_prefix(jax.random.fold_in(jax.random.fold_in(key_list[9], part), 71), part),
        "private_caches": noise(part_splits[5], (PARTICLES, SUF, LATENT), 2.0, 8.0, ((0, 4), (1, 4))),
        "new_latent": noise(part_splits[6], (PARTICLES, LATENT), 1.0, 6.0, ((0, 4),)),
        "ancestors": set_ends(jax.random.randint(part_splits[7], (PARTICLES,), 0, PARTICLES), jax.random.fold_in(part_splits[7], 1), 0, PARTICLES - 1).astype(jnp.int32),
        "lengths": set_ends(jax.random.randint(part_splits[8], (PARTICLES,), 1, SUF), jax.random.fold_in(part_splits[8], 1), 1, SUF - 1).astype(jnp.int32),
    }


masked_score = -1e30


def merge_partials(left_part, right_part):
    left_max, left_sum, left_acc = left_part
    right_max, right_sum, right_acc = right_part
    largest = jnp.maximum(left_max, right_max)
    left_factor = jnp.exp(left_max - largest)
    right_factor = jnp.exp(right_max - largest)
    return (largest, left_sum * left_factor + right_sum * right_factor,
            left_acc * left_factor[..., None] + right_acc * right_factor[..., None])


def reference(q_nope, q_rope, w_uk, w_uv, prefix, private_caches, new_latent, ancestors, lengths):
    softmax_scale = (NOPE + ROPE) ** -0.5
    latent_width = KV_RANK + ROPE
    particle_total = ancestors.shape[0]
    owners = ancestors[:, None] == jnp.arange(particle_total, dtype=jnp.int32)[None, :]
    new_lengths = jnp.sum(jnp.where(owners, lengths[None, :], 0), axis=1).astype(jnp.int32)
    migrated = private_caches[ancestors]
    positions = jnp.arange(SUF, dtype=jnp.int32)
    writes = positions[None, :] == new_lengths[:, None]
    new_caches = jnp.where(writes[:, :, None], new_latent[:, None, :], migrated)
    query_latent = jnp.einsum("phn,hnc->phc", q_nope.astype(jnp.float32), w_uk.astype(jnp.float32)).astype(jnp.bfloat16)
    queries = jnp.concatenate([query_latent, q_rope], axis=2)
    row_total = particle_total * HEADS
    flat_queries = queries.reshape(row_total, latent_width)
    start_part = (jnp.full((row_total,), masked_score, jnp.float32),
                  jnp.zeros((row_total,), jnp.float32),
                  jnp.zeros((row_total, KV_RANK), jnp.float32))

    def prefix_block(carried, key_block):
        scores = jnp.dot(flat_queries, key_block.T, preferred_element_type=jnp.float32) * softmax_scale
        block_max = jnp.max(scores, axis=1)
        weights = jnp.exp(scores - block_max[:, None])
        block_sum = jnp.sum(weights, axis=1)
        block_acc = jnp.dot(weights.astype(jnp.bfloat16), key_block[:, :KV_RANK], preferred_element_type=jnp.float32)
        return merge_partials(carried, (block_max, block_sum, block_acc)), None

    combined, unused = lax.scan(prefix_block, start_part, prefix.reshape(N_SEQ, PRE_DEV, latent_width))
    wide_queries = queries.astype(jnp.float32)
    suffix_blocks = migrated.reshape(particle_total, N_SEQ, SUF_DEV, latent_width).transpose(1, 0, 2, 3)

    def suffix_block(carried, inputs):
        key_block, block_index = inputs
        block_positions = block_index * SUF_DEV + jnp.arange(SUF_DEV, dtype=jnp.int32)
        visible = (block_positions[None, :] < new_lengths[:, None])[:, None, :]
        scores = jnp.einsum("phc,pkc->phk", wide_queries, key_block.astype(jnp.float32)) * softmax_scale
        masked = jnp.where(visible, scores, masked_score)
        block_max = jnp.max(masked, axis=2)
        weights = jnp.where(visible, jnp.exp(masked - block_max[:, :, None]), 0.0)
        block_sum = jnp.sum(weights, axis=2)
        rounded = lax.optimization_barrier(weights.astype(jnp.bfloat16)).astype(jnp.float32)
        block_acc = jnp.einsum("phk,pkc->phc", rounded, key_block[:, :, :KV_RANK].astype(jnp.float32))
        return merge_partials(carried, (block_max.reshape(row_total), block_sum.reshape(row_total),
                                        block_acc.reshape(row_total, KV_RANK))), None

    combined, unused = lax.scan(suffix_block, combined, (suffix_blocks, jnp.arange(N_SEQ, dtype=jnp.int32)))
    latent_out = (combined[2] / combined[1][:, None]).astype(jnp.bfloat16).reshape(particle_total, HEADS, KV_RANK)
    head_values = jnp.einsum("phc,hcv->phv", latent_out.astype(jnp.float32), w_uv.astype(jnp.float32)).astype(jnp.bfloat16)
    return head_values, new_caches
```

```python
import functools

import jax
import jax.numpy as jnp
from jax import lax
from jax.experimental import pallas as pl
from jax.experimental.pallas import tpu as pltpu
from jax.sharding import PartitionSpec as P

ROPE = 64
NOPE = 128

MASKED = -1e30
KEY_TILE = 512


def partner(index, step, count):
    if count & (count - 1):
        raise ValueError("seq size")
    other = index
    bit = 1
    while bit <= step:
        if step & bit:
            other = other + bit - 2 * bit * lax.rem(index // bit, 2)
        bit *= 2
    return other


def attention_kernel(
    n_seq, n_dom, scale,
    anc_ref, len_ref, q_ref, prefix_hbm, cache_ref, fresh_ref,
    latent_ref, caches_ref,
    queries, prefix, blocks, suffix, scores, acc, stats,
    send_acc, send_stat, recv_acc, recv_stat,
    load_sem, q_send, q_recv, z_send, z_recv, a_send, a_recv, s_send, s_recv,
):
    me = lax.axis_index("seq")
    dom = lax.axis_index("dom")
    local = cache_ref.shape[0]
    rows_suffix = cache_ref.shape[1]
    width = cache_ref.shape[2]
    rows = q_ref.shape[0]
    heads = rows // local
    rank = latent_ref.shape[1]
    keys = prefix.shape[0]
    group = 2 if n_seq % 2 == 0 else 1

    load = pltpu.make_async_copy(prefix_hbm, prefix, load_sem)
    load.start()

    barrier = pltpu.get_barrier_semaphore()
    for step in range(1, n_seq):
        pl.semaphore_signal(barrier, inc=1, device_id={"seq": partner(me, step, n_seq)})

    @pl.when(dom > 0)
    def _():
        pl.semaphore_signal(barrier, inc=1, device_id={"dom": dom - 1})

    @pl.when(dom < n_dom - 1)
    def _():
        pl.semaphore_signal(barrier, inc=1, device_id={"dom": dom + 1})

    below = lax.div(dom + n_dom - 1, n_dom)
    above = lax.div(2 * n_dom - 2 - dom, n_dom)
    pl.semaphore_wait(barrier, n_seq - 1 + below + above)

    def q_copy(step):
        return pltpu.make_async_remote_copy(
            src_ref=q_ref, dst_ref=queries.at[step],
            send_sem=q_send.at[step], recv_sem=q_recv.at[step],
            device_id={"seq": partner(me, step, n_seq)},
        )

    def z_copy(way, step):
        block = dom - step if way == 0 else dom + step
        view = blocks.at[pl.ds(block * local, local)]
        return pltpu.make_async_remote_copy(
            src_ref=cache_ref if step == 0 else view, dst_ref=view,
            send_sem=z_send.at[way, step], recv_sem=z_recv.at[way, step],
            device_id={"dom": dom + 1 if way == 0 else dom - 1},
        )

    def z_arrival(way, step):
        block = dom - step - 1 if way == 0 else dom + step + 1
        view = blocks.at[pl.ds(block * local, local)]
        return pltpu.make_async_remote_copy(
            src_ref=view, dst_ref=view,
            send_sem=z_send.at[way, step], recv_sem=z_recv.at[way, step],
            device_id={"dom": dom + 1 if way == 0 else dom - 1},
        )

    def z_sends(way, step):
        if way == 0:
            return (dom >= step) & (dom < n_dom - 1)
        return (dom + step < n_dom) & (dom > 0)

    def z_receives(way, step):
        if way == 0:
            return dom >= step + 1
        return dom + step + 1 < n_dom

    def z_stage(step):
        for way in (0, 1):
            if step > 0:
                @pl.when(z_receives(way, step - 1))
                def _():
                    z_arrival(way, step - 1).wait_recv()
            if step < n_dom - 1:
                @pl.when(z_sends(way, step))
                def _():
                    z_copy(way, step).start()

    for step in range(1, n_seq):
        q_copy(step).start()
    z_stage(0)
    queries[0] = q_ref[...]
    blocks[pl.ds(dom * local, local)] = cache_ref[...]
    load.wait()
    stage = 1

    for first in range(0, n_seq, group):
        for step in range(max(first, 1), first + group):
            q_copy(step).wait_recv()
        wide = group * rows
        flat = queries[first : first + group].reshape(wide, width)
        peak = jnp.full((wide, 128), MASKED, jnp.float32)
        for tile in range(keys // KEY_TILE):
            part = lax.dot_general(
                flat, prefix[tile * KEY_TILE : (tile + 1) * KEY_TILE],
                (((1,), (1,)), ((), ())), preferred_element_type=jnp.float32,
            ) * scale
            scores[:, tile * KEY_TILE : (tile + 1) * KEY_TILE] = part
            for lane in range(KEY_TILE // 128):
                peak = jnp.maximum(peak, part[:, lane * 128 : (lane + 1) * 128])
        top = jnp.max(peak, axis=1, keepdims=True)
        mass = jnp.zeros((wide, 128), jnp.float32)
        for tile in range(keys // KEY_TILE):
            weights = jnp.exp(scores[:, tile * KEY_TILE : (tile + 1) * KEY_TILE] - top)
            for lane in range(KEY_TILE // 128):
                mass = mass + weights[:, lane * 128 : (lane + 1) * 128]
            update = jnp.dot(
                weights.astype(jnp.bfloat16),
                prefix[tile * KEY_TILE : (tile + 1) * KEY_TILE, :rank],
                preferred_element_type=jnp.float32,
            )
            here = pl.ds(first * rows, wide)
            if tile == 0:
                acc[here] = update
            else:
                acc[here] += update
        total = jnp.sum(mass, axis=1, keepdims=True)
        stats[0, pl.ds(first * rows, wide)] = jnp.broadcast_to(top, (wide, 128))
        stats[1, pl.ds(first * rows, wide)] = jnp.broadcast_to(total, (wide, 128))
        if stage < n_dom:
            z_stage(stage)
            stage += 1
    while stage < n_dom:
        z_stage(stage)
        stage += 1

    place = me * rows_suffix + lax.broadcasted_iota(jnp.int32, (rows_suffix, width), 0)
    for p in range(local):
        source = anc_ref[p]
        length = len_ref[source]
        moved = blocks[source]
        suffix[p * rows_suffix : (p + 1) * rows_suffix] = moved
        fresh = jnp.broadcast_to(fresh_ref[p : p + 1].astype(jnp.float32), (rows_suffix, width))
        caches_ref[p] = jnp.where(place == length, fresh, moved.astype(jnp.float32)).astype(
            caches_ref.dtype
        )

    span = local * rows_suffix
    wide = group * rows
    row_p = lax.rem(lax.broadcasted_iota(jnp.int32, (wide, span), 0), rows) // heads
    column = lax.broadcasted_iota(jnp.int32, (wide, span), 1)
    visible = jnp.zeros((wide, span), jnp.bool_)
    for p in range(local):
        limit = jnp.clip(len_ref[anc_ref[p]] - me * rows_suffix, 0, rows_suffix)
        visible = visible | (
            (row_p == p) & (column >= p * rows_suffix) & (column < p * rows_suffix + limit)
        )

    def a_copy(step):
        return pltpu.make_async_remote_copy(
            src_ref=send_acc.at[step], dst_ref=recv_acc.at[step],
            send_sem=a_send.at[step], recv_sem=a_recv.at[step],
            device_id={"seq": partner(me, step, n_seq)},
        )

    def s_copy(step):
        return pltpu.make_async_remote_copy(
            src_ref=send_stat.at[step], dst_ref=recv_stat.at[step],
            send_sem=s_send.at[step], recv_sem=s_recv.at[step],
            device_id={"seq": partner(me, step, n_seq)},
        )

    lane = lax.broadcasted_iota(jnp.int32, (rows, 128), 1)
    for first in range(n_seq - group, -1, -group):
        here = pl.ds(first * rows, wide)
        flat = queries[first : first + group].reshape(wide, width)
        raw = lax.dot_general(
            flat, suffix[...], (((1,), (1,)), ((), ())), preferred_element_type=jnp.float32
        ) * scale
        masked = jnp.where(visible, raw, MASKED)
        old_top = stats[0, here][:, :1]
        top = jnp.maximum(old_top, jnp.max(masked, axis=1, keepdims=True))
        keep = jnp.exp(old_top - top)
        weights = jnp.where(visible, jnp.exp(masked - top), 0.0)
        total = stats[1, here][:, :1] * keep + jnp.sum(weights, axis=1, keepdims=True)
        final = acc[here] * keep + jnp.dot(
            weights.astype(jnp.bfloat16), suffix[:, :rank], preferred_element_type=jnp.float32
        )
        for offset in range(group - 1, -1, -1):
            step = first + offset
            mine = slice(offset * rows, (offset + 1) * rows)
            if step == 0:
                acc[pl.ds(0, rows)] = final[mine]
                stats[0, pl.ds(0, rows)] = jnp.broadcast_to(top[mine], (rows, 128))
                stats[1, pl.ds(0, rows)] = jnp.broadcast_to(total[mine], (rows, 128))
            else:
                send_acc[step] = final[mine].astype(jnp.bfloat16)
                packed = jnp.where(lane == 0, top[mine], total[mine])
                send_stat[step] = packed.T[:8, :]
                s_copy(step).start()
                a_copy(step).start()

    tops = [stats[0, pl.ds(0, rows)][:, :1]]
    totals = [stats[1, pl.ds(0, rows)][:, :1]]
    for step in range(1, n_seq):
        s_copy(step).wait_recv()
        got = jnp.concatenate(
            [recv_stat[step], jnp.zeros((120, rows), jnp.float32)], axis=0
        ).T
        tops.append(got[:, 0:1])
        totals.append(got[:, 1:2])
    largest = functools.reduce(jnp.maximum, tops)
    factors = [jnp.exp(t - largest) for t in tops]
    denominator = functools.reduce(jnp.add, [f * t for f, t in zip(factors, totals)])
    inverse = 1.0 / denominator
    result = acc[pl.ds(0, rows)] * (factors[0] * inverse)
    for step in range(1, n_seq):
        a_copy(step).wait_recv()
        result = result + recv_acc[step].astype(jnp.float32) * (factors[step] * inverse)
    latent_ref[...] = result.astype(latent_ref.dtype)

    for step in range(1, n_seq):
        q_copy(step).wait_send()
        a_copy(step).wait_send()
        s_copy(step).wait_send()
    for way in (0, 1):
        for step in range(n_dom - 1):
            @pl.when(z_sends(way, step))
            def _():
                z_copy(way, step).wait_send()


def on_device(
    n_seq, n_dom, q_nope, q_rope, w_uk, w_uv, prefix, private_caches, new_latent, ancestors, lengths
):
    scale = (NOPE + ROPE) ** (-0.5)
    local = ancestors.shape[0]
    rows_suffix, width = private_caches.shape[1:]
    own_heads, rank = w_uv.shape[:2]
    rows = local * own_heads
    padded = -(-rows // 128) * 128
    query_latent = jnp.einsum(
        "phn,hnc->phc", q_nope, w_uk, preferred_element_type=jnp.float32
    ).astype(jnp.bfloat16)
    own = jnp.concatenate([query_latent, q_rope], axis=2)
    if padded != rows:
        extra = padded // local - own_heads
        own = jnp.pad(own, ((0, 0), (0, extra), (0, 0)))
    own = own.reshape(padded, width)
    group = 2 if n_seq % 2 == 0 else 1
    vmem = pl.BlockSpec(memory_space=pltpu.VMEM)
    smem = pl.BlockSpec(memory_space=pltpu.SMEM)
    latent, new_caches = pl.pallas_call(
        functools.partial(attention_kernel, n_seq, n_dom, scale),
        out_shape=(
            jax.ShapeDtypeStruct((padded, rank), jnp.bfloat16),
            jax.ShapeDtypeStruct(private_caches.shape, jnp.bfloat16),
        ),
        in_specs=[smem, smem, vmem, pl.BlockSpec(memory_space=pl.ANY), vmem, vmem],
        out_specs=(vmem, vmem),
        scratch_shapes=[
            pltpu.VMEM((n_seq, padded, width), jnp.bfloat16),
            pltpu.VMEM(prefix.shape, jnp.bfloat16),
            pltpu.VMEM((n_dom * local, rows_suffix, width), jnp.bfloat16),
            pltpu.VMEM((local * rows_suffix, width), jnp.bfloat16),
            pltpu.VMEM((group * padded, prefix.shape[0]), jnp.float32),
            pltpu.VMEM((n_seq * padded, rank), jnp.float32),
            pltpu.VMEM((2, n_seq * padded, 128), jnp.float32),
            pltpu.VMEM((n_seq, padded, rank), jnp.bfloat16),
            pltpu.VMEM((n_seq, 8, padded), jnp.float32),
            pltpu.VMEM((n_seq, padded, rank), jnp.bfloat16),
            pltpu.VMEM((n_seq, 8, padded), jnp.float32),
            pltpu.SemaphoreType.DMA,
            pltpu.SemaphoreType.DMA((n_seq,)),
            pltpu.SemaphoreType.DMA((n_seq,)),
            pltpu.SemaphoreType.DMA((2, n_dom)),
            pltpu.SemaphoreType.DMA((2, n_dom)),
            pltpu.SemaphoreType.DMA((n_seq,)),
            pltpu.SemaphoreType.DMA((n_seq,)),
            pltpu.SemaphoreType.DMA((n_seq,)),
            pltpu.SemaphoreType.DMA((n_seq,)),
        ],
        compiler_params=pltpu.CompilerParams(
            collective_id=0, has_side_effects=True, vmem_limit_bytes=56 * 1024 * 1024
        ),
        name="resample_attention",
    )(ancestors, lengths, own, prefix, private_caches, new_latent)
    latent = latent.reshape(local, padded // local, rank)[:, :own_heads]
    head_values = jnp.einsum(
        "phc,hcv->phv", latent, w_uv, preferred_element_type=jnp.float32
    ).astype(jnp.bfloat16)
    return (head_values, new_caches)


def solution(mesh):
    placed = (
        P(("group", "dom"), "seq", None),
        P(("group", "dom"), "seq", None),
        P("seq", None, None),
        P("seq", None, None),
        P(("group", "seq"), None),
        P(("group", "dom"), "seq", None),
        P(("group", "dom"), None),
        P(("group", "dom")),
        P("group"),
    )
    return jax.shard_map(
        functools.partial(on_device, mesh.shape["seq"], mesh.shape["dom"]),
        mesh=mesh,
        in_specs=placed,
        out_specs=(P(("group", "dom"), "seq", None), P(("group", "dom"), "seq", None)),
        check_vma=False,
    )
```

```python
import functools

import jax
import jax.numpy as jnp
from jax import lax
from jax.experimental import pallas as pl
from jax.experimental.pallas import tpu as pltpu
from jax.sharding import PartitionSpec as P

ROPE = 64
NOPE = 128

MASKED = -1e30
KEY_TILE = 512


def partner(index, step, count):
    if count & (count - 1):
        raise ValueError("seq size")
    other = index
    bit = 1
    while bit <= step:
        if step & bit:
            other = other + bit - 2 * bit * lax.rem(index // bit, 2)
        bit *= 2
    return other


def attention_kernel(
    n_seq, n_dom, scale,
    anc_ref, len_ref, anc_wide, nope_ref, rope_ref, w_hbm, prefix_hbm, cache_ref, fresh_ref,
    latent_ref, caches_ref,
    q_ref, weight, queries, prefix, raw, picked, chosen, asked, asked_scalar, suffix, scores, acc,
    stats, send_acc, send_stat, recv_acc, recv_stat,
    load_sem, q_send, q_recv, z_send, z_recv, c_send, c_recv, n_send, n_recv, n_load,
    a_send, a_recv, s_send, s_recv,
):
    me = lax.axis_index("seq")
    dom = lax.axis_index("dom")
    local = cache_ref.shape[0]
    rows_suffix = cache_ref.shape[1]
    width = cache_ref.shape[2]
    rows = q_ref.shape[0]
    heads = rows // local
    rank = latent_ref.shape[1]
    keys = prefix.shape[1]
    chunks = len(raw[0])
    thick = rows_suffix // chunks
    group = 2 if n_seq % 2 == 0 else 1

    load_w = pltpu.make_async_copy(w_hbm, weight, load_sem.at[0])
    load_w.start()
    load = pltpu.make_async_copy(prefix_hbm, prefix, load_sem.at[1])
    load.start()

    barrier = pltpu.get_barrier_semaphore()
    for step in range(1, n_seq):
        pl.semaphore_signal(barrier, inc=1, device_id={"seq": partner(me, step, n_seq)})

    @pl.when(dom > 0)
    def _():
        pl.semaphore_signal(barrier, inc=1, device_id={"dom": dom - 1})

    @pl.when(dom < n_dom - 1)
    def _():
        pl.semaphore_signal(barrier, inc=1, device_id={"dom": dom + 1})

    below = lax.div(dom + n_dom - 1, n_dom)
    above = lax.div(2 * n_dom - 2 - dom, n_dom)
    pl.semaphore_wait(barrier, n_seq - 1 + below + above)

    def q_copy(step):
        return pltpu.make_async_remote_copy(
            src_ref=q_ref, dst_ref=queries.at[step],
            send_sem=q_send.at[step], recv_sem=q_recv.at[step],
            device_id={"seq": partner(me, step, n_seq)},
        )

    def toward(way):
        return {"dom": dom + 1 if way == 0 else dom - 1}

    def z_copy(way, step, r, arrival=False):
        hop = step + 1 if arrival else step
        block = dom - hop if way == 0 else dom + hop
        view = raw[way][r].at[pl.ds(block * local, local)]
        own = cache_ref.at[:, pl.ds(r * thick, thick)]
        return pltpu.make_async_remote_copy(
            src_ref=own if hop == 0 else view, dst_ref=view,
            send_sem=z_send.at[way, step, r], recv_sem=z_recv.at[way, step, r],
            device_id=toward(way),
        )

    def c_copy(way, r):
        return pltpu.make_async_remote_copy(
            src_ref=chosen[way][r], dst_ref=picked[way][r],
            send_sem=c_send.at[way, r], recv_sem=c_recv.at[way, r],
            device_id=toward(way),
        )

    def n_copy(way):
        return pltpu.make_async_remote_copy(
            src_ref=anc_wide, dst_ref=asked.at[way],
            send_sem=n_send.at[way], recv_sem=n_recv.at[way],
            device_id=toward(1 - way),
        )

    def z_sends(way, step):
        if way == 0:
            return (dom >= step) & (dom < n_dom - 2)
        return (dom + step < n_dom) & (dom > 1)

    def z_receives(way, step):
        if way == 0:
            return (dom >= step + 1) & (dom < n_dom - 1)
        return (dom + step + 1 < n_dom) & (dom > 0)

    def selector(way):
        return dom == (n_dom - 2 if way == 0 else 1)

    def last(way):
        return dom == (n_dom - 1 if way == 0 else 0)

    def z_stage(step, r):
        for way in (0, 1):
            if step > 0:
                @pl.when(z_receives(way, step - 1))
                def _():
                    z_copy(way, step - 1, r, arrival=True).wait_recv()
            if step < n_dom - 2:
                @pl.when(z_sends(way, step))
                def _():
                    z_copy(way, step, r).start()
            else:
                @pl.when(selector(way))
                def _():
                    if r == 0:
                        n_copy(way).wait_recv()
                        down = pltpu.make_async_copy(
                            asked.at[way], asked_scalar.at[way], n_load.at[way]
                        )
                        down.start()
                        down.wait()
                    for p in range(local):
                        want = asked_scalar[way, p, 0]
                        mine = jnp.clip(want - dom * local, 0, local - 1)
                        here = (want >= dom * local) & (want < (dom + 1) * local)
                        held = cache_ref[mine, pl.ds(r * thick, thick)]
                        came = raw[way][r][want]
                        chosen[way][r][p] = jnp.where(here, held, came)
                    c_copy(way, r).start()

    for way in (0, 1):
        @pl.when(last(way))
        def _():
            n_copy(way).start()
    if n_dom > 2:
        for r in range(chunks):
            z_stage(0, r)
    stages = [(step, r) for step in range(1 if n_dom > 2 else 0, n_dom - 1) for r in range(chunks)]
    points = 2 * (n_seq // group)
    share = -(-len(stages) // points)

    def advance():
        for _ in range(share):
            if stages:
                z_stage(*stages.pop(0))

    load_w.wait()
    head_count = weight.shape[0] // nope_ref.shape[1]
    head_row = lax.rem(lax.broadcasted_iota(jnp.int32, nope_ref.shape, 0), heads)
    nope = nope_ref[...].astype(jnp.float32)
    absorbed = jnp.zeros((rows, rank), jnp.float32)
    batch = 8 if head_count % 8 == 0 else 1
    for low in range(0, head_count, batch):
        wide_q = jnp.concatenate(
            [
                jnp.where(head_row == h, nope, 0.0).astype(jnp.bfloat16)
                for h in range(low, low + batch)
            ],
            axis=1,
        )
        deep = nope_ref.shape[1]
        absorbed = absorbed + jnp.dot(
            wide_q, weight[low * deep : (low + batch) * deep], preferred_element_type=jnp.float32
        )
    q_ref[:, :rank] = absorbed.astype(jnp.bfloat16)
    q_ref[:, rank:] = rope_ref[...]
    for step in [k for k in range(2, n_seq)] + [k for k in range(1, min(2, n_seq))]:
        q_copy(step).start()
    queries[0] = q_ref[...]
    load.wait()

    for first in range(0, n_seq, group):
        for step in range(max(first, 1), first + group):
            q_copy(step).wait_recv()
        wide = group * rows
        flat = queries[first : first + group].reshape(wide, width)
        peak = jnp.full((wide, 128), MASKED, jnp.float32)
        for tile in range(keys // KEY_TILE):
            part = jnp.dot(
                flat, prefix[:, tile * KEY_TILE : (tile + 1) * KEY_TILE],
                preferred_element_type=jnp.float32,
            ) * scale
            scores[:, tile * KEY_TILE : (tile + 1) * KEY_TILE] = part
            for lane in range(KEY_TILE // 128):
                peak = jnp.maximum(peak, part[:, lane * 128 : (lane + 1) * 128])
        top = jnp.max(peak, axis=1, keepdims=True)
        advance()
        mass = jnp.zeros((wide, 128), jnp.float32)
        for tile in range(keys // KEY_TILE):
            weights = jnp.exp(scores[:, tile * KEY_TILE : (tile + 1) * KEY_TILE] - top)
            for lane in range(KEY_TILE // 128):
                mass = mass + weights[:, lane * 128 : (lane + 1) * 128]
            update = lax.dot_general(
                weights.astype(jnp.bfloat16),
                prefix[:rank, tile * KEY_TILE : (tile + 1) * KEY_TILE],
                (((1,), (1,)), ((), ())), preferred_element_type=jnp.float32,
            )
            here = pl.ds(first * rows, wide)
            if tile == 0:
                acc[here] = update
            else:
                acc[here] += update
        total = jnp.sum(mass, axis=1, keepdims=True)
        stats[0, pl.ds(first * rows, wide)] = jnp.broadcast_to(top, (wide, 128))
        stats[1, pl.ds(first * rows, wide)] = jnp.broadcast_to(total, (wide, 128))
        advance()
    while stages:
        advance()
    for way in (0, 1):
        for r in range(chunks):
            @pl.when(last(way))
            def _():
                c_copy(way, r).wait_recv()

    place = me * rows_suffix + lax.broadcasted_iota(jnp.int32, (thick, width), 0)
    for p in range(local):
        source = anc_ref[p]
        length = len_ref[source]
        fresh = jnp.broadcast_to(fresh_ref[p : p + 1].astype(jnp.float32), (thick, width))
        mine = jnp.clip(source - dom * local, 0, local - 1)
        for r in range(chunks):
            held = cache_ref[mine, pl.ds(r * thick, thick)]
            lower = jnp.where(last(0), picked[0][r][p], raw[0][r][source])
            upper = jnp.where(last(1), picked[1][r][p], raw[1][r][source])
            moved = jnp.where(
                source < dom * local, lower, jnp.where(source >= (dom + 1) * local, upper, held)
            )
            start = p * rows_suffix + r * thick
            suffix[start : start + thick] = moved
            caches_ref[p, r * thick : (r + 1) * thick] = jnp.where(
                place + r * thick == length, fresh, moved.astype(jnp.float32)
            ).astype(caches_ref.dtype)

    span = local * rows_suffix
    wide = group * rows
    row_p = lax.rem(lax.broadcasted_iota(jnp.int32, (wide, span), 0), rows) // heads
    column = lax.broadcasted_iota(jnp.int32, (wide, span), 1)
    visible = jnp.zeros((wide, span), jnp.bool_)
    for p in range(local):
        limit = jnp.clip(len_ref[anc_ref[p]] - me * rows_suffix, 0, rows_suffix)
        visible = visible | (
            (row_p == p) & (column >= p * rows_suffix) & (column < p * rows_suffix + limit)
        )

    def a_copy(step):
        return pltpu.make_async_remote_copy(
            src_ref=send_acc.at[step], dst_ref=recv_acc.at[step],
            send_sem=a_send.at[step], recv_sem=a_recv.at[step],
            device_id={"seq": partner(me, step, n_seq)},
        )

    def s_copy(step):
        return pltpu.make_async_remote_copy(
            src_ref=send_stat.at[step], dst_ref=recv_stat.at[step],
            send_sem=s_send.at[step], recv_sem=s_recv.at[step],
            device_id={"seq": partner(me, step, n_seq)},
        )

    lane = lax.broadcasted_iota(jnp.int32, (rows, 128), 1)
    for first in range(n_seq - group, -1, -group):
        here = pl.ds(first * rows, wide)
        flat = queries[first : first + group].reshape(wide, width)
        plain = lax.dot_general(
            flat, suffix[...], (((1,), (1,)), ((), ())), preferred_element_type=jnp.float32
        ) * scale
        masked = jnp.where(visible, plain, MASKED)
        old_top = stats[0, here][:, :1]
        top = jnp.maximum(old_top, jnp.max(masked, axis=1, keepdims=True))
        keep = jnp.exp(old_top - top)
        weights = jnp.where(visible, jnp.exp(masked - top), 0.0)
        total = stats[1, here][:, :1] * keep + jnp.sum(weights, axis=1, keepdims=True)
        final = acc[here] * keep + jnp.dot(
            weights.astype(jnp.bfloat16), suffix[:, :rank], preferred_element_type=jnp.float32
        )
        for offset in range(group - 1, -1, -1):
            step = first + offset
            mine = slice(offset * rows, (offset + 1) * rows)
            if step == 0:
                acc[pl.ds(0, rows)] = final[mine]
                stats[0, pl.ds(0, rows)] = jnp.broadcast_to(top[mine], (rows, 128))
                stats[1, pl.ds(0, rows)] = jnp.broadcast_to(total[mine], (rows, 128))
            else:
                send_acc[step] = final[mine].astype(jnp.bfloat16)
                packed = jnp.where(lane == 0, top[mine], total[mine])
                send_stat[step] = packed.T[:8, :]
                s_copy(step).start()
                a_copy(step).start()

    tops = [stats[0, pl.ds(0, rows)][:, :1]]
    totals = [stats[1, pl.ds(0, rows)][:, :1]]
    for step in range(1, n_seq):
        s_copy(step).wait_recv()
        got = jnp.concatenate(
            [recv_stat[step], jnp.zeros((120, rows), jnp.float32)], axis=0
        ).T
        tops.append(got[:, 0:1])
        totals.append(got[:, 1:2])
    largest = functools.reduce(jnp.maximum, tops)
    factors = [jnp.exp(t - largest) for t in tops]
    denominator = functools.reduce(jnp.add, [f * t for f, t in zip(factors, totals)])
    inverse = 1.0 / denominator
    result = acc[pl.ds(0, rows)] * (factors[0] * inverse)
    for step in range(1, n_seq):
        a_copy(step).wait_recv()
        result = result + recv_acc[step].astype(jnp.float32) * (factors[step] * inverse)
    latent_ref[...] = result.astype(latent_ref.dtype)

    for step in range(1, n_seq):
        q_copy(step).wait_send()
        a_copy(step).wait_send()
        s_copy(step).wait_send()
    for way in (0, 1):
        @pl.when(last(way))
        def _():
            n_copy(way).wait_send()

        for r in range(chunks):
            @pl.when(selector(way))
            def _():
                c_copy(way, r).wait_send()

            for step in range(n_dom - 2):
                @pl.when(z_sends(way, step))
                def _():
                    z_copy(way, step, r).wait_send()


def on_device(
    n_seq, n_dom, q_nope, q_rope, w_uk, w_uv, prefix, private_caches, new_latent, ancestors, lengths
):
    scale = (NOPE + ROPE) ** (-0.5)
    local = ancestors.shape[0]
    rows_suffix, width = private_caches.shape[1:]
    own_heads, rank = w_uv.shape[:2]
    rows = local * own_heads
    padded = -(-rows // 128) * 128
    if padded != rows:
        extra = ((0, 0), (0, padded // local - own_heads), (0, 0))
        q_nope, q_rope = jnp.pad(q_nope, extra), jnp.pad(q_rope, extra)
    q_nope = q_nope.reshape(padded, q_nope.shape[2])
    q_rope = q_rope.reshape(padded, q_rope.shape[2])
    flat_w = w_uk.reshape(-1, rank)
    keys_first = prefix.T
    chunks = 4 if rows_suffix % 64 == 0 else 1
    ask_rows = -(-local // 8) * 8
    anc_wide = jnp.broadcast_to(
        jnp.pad(ancestors, (0, ask_rows - local))[:, None], (ask_rows, 128)
    )
    held = pltpu.VMEM((n_dom * local, rows_suffix // chunks, width), jnp.bfloat16)
    some = pltpu.VMEM((local, rows_suffix // chunks, width), jnp.bfloat16)
    group = 2 if n_seq % 2 == 0 else 1
    vmem = pl.BlockSpec(memory_space=pltpu.VMEM)
    smem = pl.BlockSpec(memory_space=pltpu.SMEM)
    whole = pl.BlockSpec(memory_space=pl.ANY)
    latent, new_caches = pl.pallas_call(
        functools.partial(attention_kernel, n_seq, n_dom, scale),
        out_shape=(
            jax.ShapeDtypeStruct((padded, rank), jnp.bfloat16),
            jax.ShapeDtypeStruct(private_caches.shape, jnp.bfloat16),
        ),
        in_specs=[smem, smem, vmem, vmem, vmem, whole, whole, vmem, vmem],
        out_specs=(vmem, vmem),
        scratch_shapes=[
            pltpu.VMEM((padded, width), jnp.bfloat16),
            pltpu.VMEM(flat_w.shape, jnp.bfloat16),
            pltpu.VMEM((n_seq, padded, width), jnp.bfloat16),
            pltpu.VMEM(keys_first.shape, jnp.bfloat16),
            [[held] * chunks] * 2,
            [[some] * chunks] * 2,
            [[some] * chunks] * 2,
            pltpu.VMEM((2, ask_rows, 128), jnp.int32),
            pltpu.SMEM((2, ask_rows, 128), jnp.int32),
            pltpu.VMEM((local * rows_suffix, width), jnp.bfloat16),
            pltpu.VMEM((group * padded, prefix.shape[0]), jnp.float32),
            pltpu.VMEM((n_seq * padded, rank), jnp.float32),
            pltpu.VMEM((2, n_seq * padded, 128), jnp.float32),
            pltpu.VMEM((n_seq, padded, rank), jnp.bfloat16),
            pltpu.VMEM((n_seq, 8, padded), jnp.float32),
            pltpu.VMEM((n_seq, padded, rank), jnp.bfloat16),
            pltpu.VMEM((n_seq, 8, padded), jnp.float32),
            pltpu.SemaphoreType.DMA((2,)),
            pltpu.SemaphoreType.DMA((n_seq,)),
            pltpu.SemaphoreType.DMA((n_seq,)),
            pltpu.SemaphoreType.DMA((2, n_dom, chunks)),
            pltpu.SemaphoreType.DMA((2, n_dom, chunks)),
            pltpu.SemaphoreType.DMA((2, chunks)),
            pltpu.SemaphoreType.DMA((2, chunks)),
            pltpu.SemaphoreType.DMA((2,)),
            pltpu.SemaphoreType.DMA((2,)),
            pltpu.SemaphoreType.DMA((2,)),
            pltpu.SemaphoreType.DMA((n_seq,)),
            pltpu.SemaphoreType.DMA((n_seq,)),
            pltpu.SemaphoreType.DMA((n_seq,)),
            pltpu.SemaphoreType.DMA((n_seq,)),
        ],
        compiler_params=pltpu.CompilerParams(
            collective_id=0, has_side_effects=True, vmem_limit_bytes=56 * 1024 * 1024
        ),
        name="resample_attention",
    )(
        ancestors, lengths, anc_wide, q_nope, q_rope, flat_w, keys_first, private_caches, new_latent
    )
    latent = latent.reshape(local, padded // local, rank)[:, :own_heads]
    head_values = jnp.einsum(
        "phc,hcv->phv", latent, w_uv, preferred_element_type=jnp.float32
    ).astype(jnp.bfloat16)
    return (head_values, new_caches)


def solution(mesh):
    placed = (
        P(("group", "dom"), "seq", None),
        P(("group", "dom"), "seq", None),
        P("seq", None, None),
        P("seq", None, None),
        P(("group", "seq"), None),
        P(("group", "dom"), "seq", None),
        P(("group", "dom"), None),
        P(("group", "dom")),
        P("group"),
    )
    return jax.shard_map(
        functools.partial(on_device, mesh.shape["seq"], mesh.shape["dom"]),
        mesh=mesh,
        in_specs=placed,
        out_specs=(P(("group", "dom"), "seq", None), P(("group", "dom"), "seq", None)),
        check_vma=False,
    )
```
